32 devices in a mesh: beam: 8 (over y, x, core), tm: 4 (over z).
Axes of the slice: x: 2, y: 2, z: 4, core: 2. Of those that a mesh axis runs over, the one named last changes fastest.
Arguments:
- samples: float32 [2, 18874368], P(None, ('beam', 'tm')), parts along dimension 1, may hold values from -6 to 6
- prototype: float32 [16, 4096], replicated, may hold values from -1.5 to 1.5
Outputs:
- spectra: bfloat16 [2, 6144, 4096], P(None, 'beam', 'tm'), parts along dimension 1
The draws below stay inside these ranges and needn't reach their ends.
There are 8 independent parts, one for each index of `beam`. The reference program is written for one: setup_inputs(seed, part) draws one part's arguments, and reference() takes and returns one part's arrays. A program takes and returns all parts, laid end to end along the dimension named above; an argument that names none is the same for every part. Nothing has to cross between parts.
All inputs are finite; a program needn't handle non-finite values.
Results may differ from the reference program's by a relative error of at most 0.001.
Values may be sent and summed in bfloat16 or wider, within the bound.
A program may use at most 128 MiB of HBM per device.

```python
import math
import jax
import jax.numpy as jnp

CHANNELS = 4096
TAPS = 16
HOP = 3072
FRAMES = 768
SAMPLES = 2359296


def steps_of(rng, extent, shards, low, top_value):
    factor_of = 1.0
    for axis_at, blocks in shards:
        draws = jax.random.uniform(jax.random.fold_in(jax.random.fold_in(rng, 6), axis_at), (blocks,), jnp.float32, low / len(shards), top_value / len(shards))
        factor_of = factor_of * jnp.repeat(jnp.exp(draws), extent[axis_at] // blocks).reshape((-1,) + (1,) * (len(extent) - 1 - axis_at))
    return factor_of


def noise(own_key, dims, scale, limit, shards=(), held_as=jnp.bfloat16):
    result = jax.random.normal(own_key, dims, jnp.float32) * scale
    if len(shards) > 0:
        result = steps_of(own_key, dims, shards, -0.22, 0.18) * result
    return jnp.clip(result, min=-limit, max=limit).astype(held_as)


def setup_inputs(seed: int = 0, part: int = 0) -> dict:
    key_list = jax.random.split(jax.random.key(seed), 3)
    part_keys = jax.random.split(jax.random.fold_in(key_list[2], part), 3)
    return {
        "samples": noise(part_keys[0], (2, SAMPLES), 1.0, 6.0, ((1, 4),), jnp.float32),
        "prototype": noise(key_list[1], (TAPS, CHANNELS), TAPS ** -0.5, 1.5, (), jnp.float32),
    }


def reference(samples, prototype):
    window = TAPS * CHANNELS
    zeros_front = jnp.zeros((2, window - HOP), samples.dtype)
    extended = jnp.concatenate([zeros_front, samples], axis=1)
    signal = extended[0] + 1j * extended[1]
    frame_ids = jnp.arange(FRAMES).astype(jnp.int32)
    phase_ids = jnp.arange(CHANNELS).astype(jnp.int32)
    folded = jnp.zeros((FRAMES, CHANNELS), signal.dtype)
    for tap_index in range(TAPS):
        starts = frame_ids * HOP + tap_index * CHANNELS
        index_grid = (starts[:, None] + phase_ids[None, :]).astype(jnp.int32)
        folded = folded + prototype[tap_index][None, :] * signal[index_grid]
    transformed = jnp.fft.fft(folded, axis=1)
    rotation = (frame_ids + 1) * HOP % CHANNELS
    turns = phase_ids[None, :] * rotation[:, None] % CHANNELS
    angle = 2.0 * math.pi * turns.astype(samples.dtype) / CHANNELS
    factor = (jnp.cos(angle) - 1j * jnp.sin(angle)) / math.sqrt(CHANNELS)
    spectrum = transformed * factor
    return jnp.stack([jnp.real(spectrum), jnp.imag(spectrum)]).astype(jnp.bfloat16)
```

```python
import functools
import math

import numpy as np
import jax
import jax.numpy as jnp
from jax import lax
from jax.experimental import pallas as pl
from jax.experimental.pallas import tpu as pltpu
from jax.sharding import PartitionSpec as P

CHANNELS = 4096
TAPS = 16
HOP = 3072
LANES = 128
FIRST = 128
SECOND = CHANNELS // FIRST
ROWS = 2 * CHANNELS // LANES
HOP_ROWS = 2 * HOP // LANES
RIM = TAPS * CHANNELS - HOP
RIM_ROWS = 2 * RIM // LANES
CHUNK = 16
GROUP = 8
MESH = pl.DeviceIdType.MESH


def split_pair(table):
    high = np.asarray(table, np.float32).astype(jnp.bfloat16)
    low = (np.asarray(table, np.float64) - high.astype(np.float64)).astype(jnp.bfloat16)
    return high, low


def first_table():
    b1, a, d = np.meshgrid(np.arange(4), np.arange(32), np.arange(FIRST), indexing="ij")
    angle = 2 * np.pi * ((4 * a + b1) * d % FIRST) / FIRST
    cos, sin = np.cos(angle), np.sin(angle)
    table = np.zeros((4, 32, 2, 2, FIRST))
    table[:, :, 0, 0], table[:, :, 1, 0] = cos, sin
    table[:, :, 0, 1], table[:, :, 1, 1] = -sin, cos
    high, low = split_pair(table.reshape(2 * FIRST, 2 * FIRST))
    return np.concatenate([high, high, low], axis=0)


def middle_table():
    angle = 2 * np.pi * np.outer(np.arange(SECOND), np.arange(FIRST)) / CHANNELS
    return (np.stack([np.cos(angle), np.sin(angle)]) / math.sqrt(CHANNELS)).astype(np.float32)


def second_table():
    angle = 2 * np.pi * (np.outer(np.arange(SECOND), np.arange(SECOND)) % SECOND) / SECOND
    eye = np.eye(GROUP)
    both = np.stack([np.cos(angle), np.sin(angle)])
    table = np.einsum("kcm,tu->kctum", both, eye).reshape(2 * SECOND * GROUP, GROUP * SECOND)
    high, low = split_pair(table)
    return np.concatenate([high, high, low], axis=1)


def split_value(value):
    high = value.astype(jnp.bfloat16)
    low = (value - high.astype(jnp.float32)).astype(jnp.bfloat16)
    return high, low


def partner(me, step, count):
    if count & (count - 1):
        return lax.rem(me + step, count)
    other = me
    bit = 1
    while bit < count:
        if step & bit:
            other = other + bit * (1 - 2 * lax.rem(me // bit, 2))
        bit *= 2
    return other


def kernel(count, frames, x_ref, proto_ref, one_ref, mid_ref, two_ref, out_ref,
           ext, folded, lhs, rhs, staged, load_sem, own_sem, rim_sems, send_sems, recv_sems):
    me = lax.axis_index("tm")
    chunks = frames // CHUNK
    rim_chunks = -(-RIM // (HOP * CHUNK))
    local_rows = frames * HOP_ROWS
    width = CHANNELS // count

    load = pltpu.make_async_copy(x_ref, ext.at[pl.ds(RIM_ROWS, local_rows)], load_sem)
    load.start()

    barrier = pltpu.get_barrier_semaphore()
    for step in range(1, count):
        pl.semaphore_signal(barrier, inc=1, device_id={"tm": partner(me, step, count)}, device_id_type=MESH)
    pl.semaphore_wait(barrier, count - 1)

    def rim_copy():
        return pltpu.make_async_remote_copy(
            src_ref=x_ref.at[pl.ds(local_rows - RIM_ROWS, RIM_ROWS)],
            dst_ref=ext.at[pl.ds(0, RIM_ROWS)],
            send_sem=rim_sems.at[0],
            recv_sem=rim_sems.at[1],
            device_id={"tm": lax.rem(me + 1, count)},
            device_id_type=MESH,
        )

    @pl.when(me < count - 1)
    def _():
        rim_copy().start()

    @pl.when(me == 0)
    def _():
        ext[pl.ds(0, RIM_ROWS), :] = jnp.zeros((RIM_ROWS, LANES), jnp.float32)

    load.wait()
    order = sorted(range(1, count), key=lambda step: (step < count // 2, step))

    def chunk_step(index, carry):
        chunk = lax.rem(index + rim_chunks, chunks)

        @pl.when(jnp.logical_and(index == chunks - rim_chunks, me > 0))
        def _():
            rim_copy().wait_recv()

        base = chunk * (CHUNK * HOP_ROWS)

        def fold(v, carry):
            taps = [proto_ref[tap, pl.ds(pl.multiple_of(v * 8, 8), 8), :] for tap in range(TAPS)]
            for t in range(CHUNK):
                total = None
                for tap in range(TAPS):
                    start = pl.multiple_of(base + (HOP_ROWS * t + ROWS * tap) + v * 8, 8)
                    term = taps[tap] * ext[pl.ds(start, 8), :]
                    total = term if total is None else total + term
                turn = (t + 1) * HOP % CHANNELS * 2 // LANES // 8
                place = lax.rem(v + turn, ROWS // 8)
                folded[t, pl.ds(pl.multiple_of(place * 8, 8), 8), :] = total
            return carry

        lax.fori_loop(0, ROWS // 8, fold, 0)

        lane = lax.broadcasted_iota(jnp.int32, (ROWS, LANES), 1)
        even = lax.rem(lane // SECOND, 2) == 0
        for pair in range(CHUNK // 2):
            one, other = folded[2 * pair], folded[2 * pair + 1]
            upper = jnp.where(even, one, pltpu.roll(other, SECOND, 1))
            lower = jnp.where(even, pltpu.roll(one, LANES - SECOND, 1), other)
            turned = jnp.concatenate([upper, lower], axis=0).T
            high, low = split_value(turned)
            for side in range(2):
                rows = pl.ds((2 * pair + side) * SECOND, SECOND)
                for half in range(2):
                    start = (2 * half + side) * SECOND
                    piece = high[start:start + SECOND]
                    lhs[rows, pl.ds(half * LANES, LANES)] = piece
                    lhs[rows, pl.ds((2 + half) * LANES, LANES)] = low[start:start + SECOND]
                    lhs[rows, pl.ds((4 + half) * LANES, LANES)] = piece

        cos, sin = mid_ref[0], mid_ref[1]
        results = []
        for group in range(CHUNK // GROUP):
            size = GROUP * SECOND
            section = jnp.dot(lhs[pl.ds(group * size, size), :], one_ref[...],
                              preferred_element_type=jnp.float32)
            for t in range(GROUP):
                real = section[t * SECOND:(t + 1) * SECOND, :FIRST]
                imag = section[t * SECOND:(t + 1) * SECOND, FIRST:]
                for half, value in enumerate((real * cos + imag * sin, imag * cos - real * sin)):
                    high, low = split_value(value)
                    columns = pl.ds(half * FIRST, FIRST)
                    rhs[group, pl.ds(t * SECOND, SECOND), columns] = high
                    rhs[group, pl.ds(size + t * SECOND, SECOND), columns] = low
                    rhs[group, pl.ds(2 * size + t * SECOND, SECOND), columns] = high
            product = jnp.dot(two_ref[...], rhs[group], preferred_element_type=jnp.float32)
            results.append((product[:size, :FIRST] + product[size:, FIRST:],
                            product[:size, FIRST:] - product[size:, :FIRST]))
        for part in range(2):
            for c in range(SECOND):
                block = jnp.concatenate(
                    [results[group][part][c * GROUP:(c + 1) * GROUP] for group in range(CHUNK // GROUP)], axis=0)
                owner, at = divmod(c * FIRST, width)
                staged[chunk, owner, part, :, pl.ds(at, FIRST)] = block.astype(jnp.bfloat16)

        rows = pl.ds(pl.multiple_of(me * frames + chunk * CHUNK, CHUNK), CHUNK)
        for step in order:
            to = partner(me, step, count)
            pltpu.make_async_remote_copy(
                src_ref=staged.at[chunk, to],
                dst_ref=out_ref.at[:, rows, :],
                send_sem=send_sems.at[step - 1],
                recv_sem=recv_sems.at[step - 1],
                device_id={"tm": to},
                device_id_type=MESH,
            ).start()
        pltpu.make_async_copy(staged.at[chunk, me], out_ref.at[:, rows, :], own_sem).start()
        return carry

    lax.fori_loop(0, chunks, chunk_step, 0)

    def block_of(device):
        return out_ref.at[:, pl.ds(pl.multiple_of(device * frames, CHUNK), frames), :]

    @pl.when(me < count - 1)
    def _():
        rim_copy().wait_send()

    pltpu.make_async_copy(block_of(me), block_of(me), own_sem).wait()
    for step in order:
        source = partner(me, step, count) if not count & (count - 1) else lax.rem(me + count - step, count)
        whole = pltpu.make_async_remote_copy(
            src_ref=block_of(source),
            dst_ref=block_of(source),
            send_sem=send_sems.at[step - 1],
            recv_sem=recv_sems.at[step - 1],
            device_id={"tm": partner(me, step, count)},
            device_id_type=MESH,
        )
        whole.wait_send()
        whole.wait_recv()


def local(count, samples, prototype):
    frames = samples.shape[1] // HOP
    rows = samples.shape[1] // LANES
    interleaved = samples.reshape(2, rows, LANES).transpose(1, 0, 2).reshape(2 * rows, LANES)
    taps = jnp.repeat(prototype.reshape(TAPS, CHANNELS // LANES, LANES), 2, axis=1)
    vmem = pl.BlockSpec(memory_space=pltpu.VMEM)
    anywhere = pl.BlockSpec(memory_space=pl.ANY)
    width = CHANNELS // count
    return pl.pallas_call(
        functools.partial(kernel, count, frames),
        out_shape=jax.ShapeDtypeStruct((2, frames * count, width), jnp.bfloat16),
        in_specs=[anywhere, vmem, vmem, vmem, vmem],
        out_specs=anywhere,
        scratch_shapes=[
            pltpu.VMEM((RIM_ROWS + 2 * rows, LANES), jnp.float32),
            pltpu.VMEM((CHUNK, ROWS, LANES), jnp.float32),
            pltpu.VMEM((CHUNK * SECOND, 6 * LANES), jnp.bfloat16),
            pltpu.VMEM((CHUNK // GROUP, 3 * GROUP * SECOND, 2 * FIRST), jnp.bfloat16),
            pltpu.VMEM((frames // CHUNK, count, 2, CHUNK, width), jnp.bfloat16),
            pltpu.SemaphoreType.DMA,
            pltpu.SemaphoreType.DMA,
            pltpu.SemaphoreType.DMA((2,)),
            pltpu.SemaphoreType.DMA((count - 1,)),
            pltpu.SemaphoreType.DMA((count - 1,)),
        ],
        compiler_params=pltpu.CompilerParams(
            collective_id=0, has_side_effects=True, vmem_limit_bytes=48 * 1024 * 1024
        ),
    )(interleaved, taps, jnp.asarray(first_table()), jnp.asarray(middle_table()), jnp.asarray(second_table()))


def solution(mesh):
    count = mesh.shape["tm"]
    placed = (P(None, ("beam", "tm")), P())
    return jax.shard_map(
        functools.partial(local, count), mesh=mesh, in_specs=placed,
        out_specs=P(None, "beam", "tm"), check_vma=False,
    )
```

```python
import functools
import math

import numpy as np
import jax
import jax.numpy as jnp
from jax import lax
from jax.experimental import pallas as pl
from jax.experimental.pallas import tpu as pltpu
from jax.sharding import PartitionSpec as P

CHANNELS = 4096
TAPS = 16
HOP = 3072
LANES = 128
FIRST = 128
SECOND = CHANNELS // FIRST
ROWS = 2 * CHANNELS // LANES
HOP_ROWS = 2 * HOP // LANES
RIM = TAPS * CHANNELS - HOP
RIM_ROWS = 2 * RIM // LANES
CHUNK = 16
GROUP = 8
MESH = pl.DeviceIdType.MESH


def split_pair(table):
    high = np.asarray(table, np.float32).astype(jnp.bfloat16)
    low = (np.asarray(table, np.float64) - high.astype(np.float64)).astype(jnp.bfloat16)
    return high, low


def first_table():
    b1, a, d = np.meshgrid(np.arange(4), np.arange(32), np.arange(FIRST), indexing="ij")
    angle = 2 * np.pi * ((4 * a + b1) * d % FIRST) / FIRST
    cos, sin = np.cos(angle), np.sin(angle)
    table = np.zeros((4, 32, 2, 2, FIRST))
    table[:, :, 0, 0], table[:, :, 1, 0] = cos, sin
    table[:, :, 0, 1], table[:, :, 1, 1] = -sin, cos
    high, low = split_pair(table.reshape(2 * FIRST, 2 * FIRST))
    return np.concatenate([high, high, low], axis=0)


def middle_table():
    angle = 2 * np.pi * np.outer(np.arange(SECOND), np.arange(FIRST)) / CHANNELS
    return (np.stack([np.cos(angle), np.sin(angle)]) / math.sqrt(CHANNELS)).astype(np.float32)


def second_table():
    angle = 2 * np.pi * (np.outer(np.arange(SECOND), np.arange(SECOND)) % SECOND) / SECOND
    eye = np.eye(GROUP)
    both = np.stack([np.cos(angle), np.sin(angle)])
    table = np.einsum("kcm,tu->kctum", both, eye).reshape(2 * SECOND * GROUP, GROUP * SECOND)
    high, low = split_pair(table)
    return np.concatenate([high, high, low], axis=1)


def split_value(value):
    high = value.astype(jnp.bfloat16)
    low = (value - high.astype(jnp.float32)).astype(jnp.bfloat16)
    return high, low


def partner(me, step, count):
    if count & (count - 1):
        return lax.rem(me + step, count)
    other = me
    bit = 1
    while bit < count:
        if step & bit:
            other = other + bit * (1 - 2 * lax.rem(me // bit, 2))
        bit *= 2
    return other


def kernel(count, frames, x_hbm, proto_hbm, one_hbm, mid_hbm, two_hbm, out_ref,
           ext, raw, spread, proto_ref, one_ref, mid_ref, two_ref, folded, lhs, rhs, staged,
           load_sems, own_sem, rim_sems, head_sems, send_sems, recv_sems):
    me = lax.axis_index("tm")
    chunks = frames // CHUNK
    local_rows = frames * HOP_ROWS
    head_rows = CHUNK * HOP_ROWS
    past_rows = RIM_ROWS - head_rows
    width = CHANNELS // count

    loads = [
        pltpu.make_async_copy(source, target, load_sems.at[at])
        for at, (source, target) in enumerate((
            (proto_hbm, raw),
            (x_hbm, ext.at[pl.ds(RIM_ROWS, local_rows)]),
            (one_hbm, one_ref),
            (mid_hbm, mid_ref),
            (two_hbm, two_ref),
        ))
    ]
    for load in loads:
        load.start()

    barrier = pltpu.get_barrier_semaphore()
    for step in range(1, count):
        pl.semaphore_signal(barrier, inc=1, device_id={"tm": partner(me, step, count)}, device_id_type=MESH)
    pl.semaphore_wait(barrier, count - 1)

    def past_copy():
        return pltpu.make_async_remote_copy(
            src_ref=x_hbm.at[pl.ds(local_rows - past_rows, past_rows)],
            dst_ref=ext.at[pl.ds(head_rows, past_rows)],
            send_sem=rim_sems.at[0],
            recv_sem=rim_sems.at[1],
            device_id={"tm": lax.rem(me + 1, count)},
            device_id_type=MESH,
        )

    def head_copy():
        return pltpu.make_async_remote_copy(
            src_ref=x_hbm.at[pl.ds(0, head_rows)],
            dst_ref=ext.at[pl.ds(RIM_ROWS + local_rows, head_rows)],
            send_sem=head_sems.at[0],
            recv_sem=head_sems.at[1],
            device_id={"tm": lax.rem(me + count - 1, count)},
            device_id_type=MESH,
        )

    @pl.when(me < count - 1)
    def _():
        past_copy().start()

    @pl.when(me > 0)
    def _():
        head_copy().start()

    @pl.when(me == 0)
    def _():
        ext[pl.ds(0, RIM_ROWS), :] = jnp.zeros((RIM_ROWS, LANES), jnp.float32)

    loads[0].wait()
    for row in range(ROWS):
        spread[pl.ds(row * TAPS, TAPS), :] = raw[:, pl.ds(row // 2 * LANES, LANES)]
    for tap in range(TAPS):
        for v in range(ROWS // 8):
            proto_ref[tap, pl.ds(v * 8, 8), :] = spread[pl.ds(v * 8 * TAPS + tap, 8, stride=TAPS), :]
    for load in loads[1:]:
        load.wait()
    order = sorted(range(1, count), key=lambda step: (step < count // 2, step))

    def chunk_step(index, carry):
        late = chunks - 2
        chunk = jnp.where(index < late, index + 2,
                          jnp.where(index == late, 1, jnp.where(index == late + 1, chunks, 0)))

        @pl.when(jnp.logical_and(index == late, me > 0))
        def _():
            past_copy().wait_recv()

        @pl.when(index == late + 1)
        def _():
            head_copy().wait_recv()

        base = chunk * (CHUNK * HOP_ROWS)

        def fold(v, carry):
            taps = [proto_ref[tap, pl.ds(pl.multiple_of(v * 8, 8), 8), :] for tap in range(TAPS)]
            for t in range(CHUNK):
                total = None
                for tap in range(TAPS):
                    start = pl.multiple_of(base + (HOP_ROWS * t + ROWS * tap) + v * 8, 8)
                    term = taps[tap] * ext[pl.ds(start, 8), :]
                    total = term if total is None else total + term
                turn = (t + 1) * HOP % CHANNELS * 2 // LANES // 8
                place = lax.rem(v + turn, ROWS // 8)
                folded[t, pl.ds(pl.multiple_of(place * 8, 8), 8), :] = total
            return carry

        lax.fori_loop(0, ROWS // 8, fold, 0)

        lane = lax.broadcasted_iota(jnp.int32, (ROWS, LANES), 1)
        even = lax.rem(lane // SECOND, 2) == 0
        for pair in range(CHUNK // 2):
            one, other = folded[2 * pair], folded[2 * pair + 1]
            upper = jnp.where(even, one, pltpu.roll(other, SECOND, 1))
            lower = jnp.where(even, pltpu.roll(one, LANES - SECOND, 1), other)
            turned = jnp.concatenate([upper, lower], axis=0).T
            high, low = split_value(turned)
            for side in range(2):
                rows = pl.ds((2 * pair + side) * SECOND, SECOND)
                for half in range(2):
                    start = (2 * half + side) * SECOND
                    piece = high[start:start + SECOND]
                    lhs[rows, pl.ds(half * LANES, LANES)] = piece
                    lhs[rows, pl.ds((2 + half) * LANES, LANES)] = low[start:start + SECOND]
                    lhs[rows, pl.ds((4 + half) * LANES, LANES)] = piece

        cos, sin = mid_ref[0], mid_ref[1]
        results = []
        for group in range(CHUNK // GROUP):
            size = GROUP * SECOND
            section = jnp.dot(lhs[pl.ds(group * size, size), :], one_ref[...],
                              preferred_element_type=jnp.float32)
            for t in range(GROUP):
                real = section[t * SECOND:(t + 1) * SECOND, :FIRST]
                imag = section[t * SECOND:(t + 1) * SECOND, FIRST:]
                for half, value in enumerate((real * cos + imag * sin, imag * cos - real * sin)):
                    high, low = split_value(value)
                    columns = pl.ds(half * FIRST, FIRST)
                    rhs[group, pl.ds(t * SECOND, SECOND), columns] = high
                    rhs[group, pl.ds(size + t * SECOND, SECOND), columns] = low
                    rhs[group, pl.ds(2 * size + t * SECOND, SECOND), columns] = high
            product = jnp.dot(two_ref[...], rhs[group], preferred_element_type=jnp.float32)
            results.append((product[:size, :FIRST] + product[size:, FIRST:],
                            product[:size, FIRST:] - product[size:, :FIRST]))
        for part in range(2):
            for c in range(SECOND):
                block = jnp.concatenate(
                    [results[group][part][c * GROUP:(c + 1) * GROUP] for group in range(CHUNK // GROUP)], axis=0)
                owner, at = divmod(c * FIRST, width)
                staged[chunk, owner, part, :, pl.ds(at, FIRST)] = block.astype(jnp.bfloat16)

        rows = pl.ds(pl.multiple_of(me * frames + chunk * CHUNK, CHUNK), CHUNK)
        for step in order:
            to = partner(me, step, count)
            pltpu.make_async_remote_copy(
                src_ref=staged.at[chunk, to],
                dst_ref=out_ref.at[:, rows, :],
                send_sem=send_sems.at[step - 1],
                recv_sem=recv_sems.at[step - 1],
                device_id={"tm": to},
                device_id_type=MESH,
            ).start()
        pltpu.make_async_copy(staged.at[chunk, me], out_ref.at[:, rows, :], own_sem).start()
        return carry

    total = chunks - 1 + jnp.where(me < count - 1, 1, 0) + jnp.where(me == 0, 1, 0)
    lax.fori_loop(0, total, chunk_step, 0)

    @pl.when(me < count - 1)
    def _():
        past_copy().wait_send()

    @pl.when(me > 0)
    def _():
        head_copy().wait_send()

    def each_range(device, act):
        first, last = device == 0, device == count - 1
        for chosen, skip, size in (
            (first, 0, frames + CHUNK),
            (last, CHUNK, frames - CHUNK),
            (jnp.logical_not(jnp.logical_or(first, last)), CHUNK, frames),
        ):
            @pl.when(chosen)
            def _():
                act(out_ref.at[:, pl.ds(pl.multiple_of(device * frames + skip, CHUNK), size), :])

    each_range(me, lambda rows: pltpu.make_async_copy(rows, rows, own_sem).wait())
    for step in order:
        to = partner(me, step, count)
        source = to if not count & (count - 1) else lax.rem(me + count - step, count)

        def described(rows):
            return pltpu.make_async_remote_copy(
                src_ref=rows, dst_ref=rows, send_sem=send_sems.at[step - 1],
                recv_sem=recv_sems.at[step - 1], device_id={"tm": to}, device_id_type=MESH)

        each_range(me, lambda rows: described(rows).wait_send())
        each_range(source, lambda rows: described(rows).wait_recv())


def local(count, samples, prototype):
    frames = samples.shape[1] // HOP
    rows = samples.shape[1] // LANES
    interleaved = samples.reshape(2, rows, LANES).transpose(1, 0, 2).reshape(2 * rows, LANES)
    one, middle, two = first_table(), middle_table(), second_table()
    in_hbm = pl.BlockSpec(memory_space=pltpu.HBM)
    anywhere = pl.BlockSpec(memory_space=pl.ANY)
    width = CHANNELS // count
    return pl.pallas_call(
        functools.partial(kernel, count, frames),
        out_shape=jax.ShapeDtypeStruct((2, frames * count, width), jnp.bfloat16),
        in_specs=[in_hbm] * 5,
        out_specs=anywhere,
        scratch_shapes=[
            pltpu.VMEM((RIM_ROWS + 2 * rows + CHUNK * HOP_ROWS, LANES), jnp.float32),
            pltpu.VMEM(prototype.shape, jnp.float32),
            pltpu.VMEM((ROWS * TAPS, LANES), jnp.float32),
            pltpu.VMEM((TAPS, ROWS, LANES), jnp.float32),
            pltpu.VMEM(one.shape, one.dtype),
            pltpu.VMEM(middle.shape, middle.dtype),
            pltpu.VMEM(two.shape, two.dtype),
            pltpu.VMEM((CHUNK, ROWS, LANES), jnp.float32),
            pltpu.VMEM((CHUNK * SECOND, 6 * LANES), jnp.bfloat16),
            pltpu.VMEM((CHUNK // GROUP, 3 * GROUP * SECOND, 2 * FIRST), jnp.bfloat16),
            pltpu.VMEM((frames // CHUNK + 1, count, 2, CHUNK, width), jnp.bfloat16),
            pltpu.SemaphoreType.DMA((5,)),
            pltpu.SemaphoreType.DMA,
            pltpu.SemaphoreType.DMA((2,)),
            pltpu.SemaphoreType.DMA((2,)),
            pltpu.SemaphoreType.DMA((count - 1,)),
            pltpu.SemaphoreType.DMA((count - 1,)),
        ],
        compiler_params=pltpu.CompilerParams(
            collective_id=0, has_side_effects=True, vmem_limit_bytes=60300000
        ),
    )(interleaved, prototype, jnp.asarray(one), jnp.asarray(middle), jnp.asarray(two))


def solution(mesh):
    count = mesh.shape["tm"]
    placed = (P(None, ("beam", "tm")), P())
    return jax.shard_map(
        functools.partial(local, count), mesh=mesh, in_specs=placed,
        out_specs=P(None, "beam", "tm"), check_vma=False,
    )
```

```python
import functools
import math

import numpy as np
import jax
import jax.numpy as jnp
from jax import lax
from jax.experimental import pallas as pl
from jax.experimental.pallas import tpu as pltpu
from jax.sharding import PartitionSpec as P

CHANNELS = 4096
TAPS = 16
HOP = 3072
LANES = 128
FIRST = 128
SECOND = CHANNELS // FIRST
ROWS = 2 * CHANNELS // LANES
HOP_ROWS = 2 * HOP // LANES
RIM = TAPS * CHANNELS - HOP
RIM_ROWS = 2 * RIM // LANES
CHUNK = 16
GROUP = 8
MESH = pl.DeviceIdType.MESH


def split_pair(table):
    high = np.asarray(table, np.float32).astype(jnp.bfloat16)
    low = (np.asarray(table, np.float64) - high.astype(np.float64)).astype(jnp.bfloat16)
    return high, low


def first_table():
    b1, a, d = np.meshgrid(np.arange(4), np.arange(32), np.arange(FIRST), indexing="ij")
    angle = 2 * np.pi * ((4 * a + b1) * d % FIRST) / FIRST
    cos, sin = np.cos(angle), np.sin(angle)
    table = np.zeros((4, 32, 2, 2, FIRST))
    table[:, :, 0, 0], table[:, :, 1, 0] = cos, sin
    table[:, :, 0, 1], table[:, :, 1, 1] = -sin, cos
    high, low = split_pair(table.reshape(2 * FIRST, 2 * FIRST))
    return np.concatenate([high, high, low], axis=0)


def middle_table():
    angle = 2 * np.pi * np.outer(np.arange(SECOND), np.arange(FIRST)) / CHANNELS
    return (np.stack([np.cos(angle), np.sin(angle)]) / math.sqrt(CHANNELS)).astype(np.float32)


def second_table():
    angle = 2 * np.pi * (np.outer(np.arange(SECOND), np.arange(SECOND)) % SECOND) / SECOND
    eye = np.eye(GROUP)
    both = np.stack([np.cos(angle), np.sin(angle)])
    table = np.einsum("kcm,tu->kctum", both, eye).reshape(2 * SECOND * GROUP, GROUP * SECOND)
    high, low = split_pair(table)
    return np.concatenate([high, high, low], axis=1)


def split_value(value):
    high = value.astype(jnp.bfloat16)
    low = (value - high.astype(jnp.float32)).astype(jnp.bfloat16)
    return high, low


def partner(me, step, count):
    if count & (count - 1):
        return lax.rem(me + step, count)
    other = me
    bit = 1
    while bit < count:
        if step & bit:
            other = other + bit * (1 - 2 * lax.rem(me // bit, 2))
        bit *= 2
    return other


def kernel(count, frames, x_hbm, proto_hbm, one_hbm, mid_hbm, two_hbm, out_ref,
           ext, raw, spread, proto_ref, one_ref, mid_ref, two_ref, folded, lhs, rhs, staged,
           load_sems, own_sem, rim_sems, head_sems, send_sems, recv_sems):
    me = lax.axis_index("tm")
    chunks = frames // CHUNK
    local_rows = frames * HOP_ROWS
    head_rows = CHUNK * HOP_ROWS
    past_rows = RIM_ROWS - head_rows
    width = CHANNELS // count

    loads = [
        pltpu.make_async_copy(source, target, load_sems.at[at])
        for at, (source, target) in enumerate((
            (proto_hbm, raw),
            (x_hbm, ext.at[pl.ds(RIM_ROWS, local_rows)]),
            (one_hbm, one_ref),
            (mid_hbm, mid_ref),
            (two_hbm, two_ref),
        ))
    ]
    for load in loads:
        load.start()

    barrier = pltpu.get_barrier_semaphore()
    for step in range(1, count):
        pl.semaphore_signal(barrier, inc=1, device_id={"tm": partner(me, step, count)}, device_id_type=MESH)
    pl.semaphore_wait(barrier, count - 1)

    def past_copy():
        return pltpu.make_async_remote_copy(
            src_ref=x_hbm.at[pl.ds(local_rows - past_rows, past_rows)],
            dst_ref=ext.at[pl.ds(head_rows, past_rows)],
            send_sem=rim_sems.at[0],
            recv_sem=rim_sems.at[1],
            device_id={"tm": lax.rem(me + 1, count)},
            device_id_type=MESH,
        )

    def head_copy():
        return pltpu.make_async_remote_copy(
            src_ref=x_hbm.at[pl.ds(0, head_rows)],
            dst_ref=ext.at[pl.ds(RIM_ROWS + local_rows, head_rows)],
            send_sem=head_sems.at[0],
            recv_sem=head_sems.at[1],
            device_id={"tm": lax.rem(me + count - 1, count)},
            device_id_type=MESH,
        )

    @pl.when(me < count - 1)
    def _():
        past_copy().start()

    @pl.when(me > 0)
    def _():
        head_copy().start()

    @pl.when(me == 0)
    def _():
        ext[pl.ds(0, RIM_ROWS), :] = jnp.zeros((RIM_ROWS, LANES), jnp.float32)

    loads[0].wait()
    for row in range(ROWS):
        spread[pl.ds(row * TAPS, TAPS), :] = raw[:, pl.ds(row // 2 * LANES, LANES)]
    for tap in range(TAPS):
        for v in range(ROWS // 8):
            proto_ref[tap, pl.ds(v * 8, 8), :] = spread[pl.ds(v * 8 * TAPS + tap, 8, stride=TAPS), :]
    for load in loads[1:]:
        load.wait()
    order = sorted(range(1, count), key=lambda step: (step < count // 2, step))

    def chunk_step(index, carry):
        late = chunks - 2
        chunk = jnp.where(index < late, index + 2,
                          jnp.where(index == late, 1, jnp.where(index == late + 1, chunks, 0)))

        @pl.when(jnp.logical_and(index == late, me > 0))
        def _():
            past_copy().wait_recv()

        @pl.when(index == late + 1)
        def _():
            head_copy().wait_recv()

        base = chunk * (CHUNK * HOP_ROWS)

        def fold(v, carry):
            taps = [proto_ref[tap, pl.ds(pl.multiple_of(v * 8, 8), 8), :] for tap in range(TAPS)]
            for t in range(CHUNK):
                total = None
                for tap in range(TAPS):
                    start = pl.multiple_of(base + (HOP_ROWS * t + ROWS * tap) + v * 8, 8)
                    term = taps[tap] * ext[pl.ds(start, 8), :]
                    total = term if total is None else total + term
                turn = (t + 1) * HOP % CHANNELS * 2 // LANES // 8
                place = lax.rem(v + turn, ROWS // 8)
                folded[t, pl.ds(pl.multiple_of(place * 8, 8), 8), :] = total
            return carry

        lax.fori_loop(0, ROWS // 8, fold, 0)

        lane = lax.broadcasted_iota(jnp.int32, (ROWS, LANES), 1)
        even = lax.rem(lane // SECOND, 2) == 0
        for pair in range(CHUNK // 2):
            one, other = folded[2 * pair], folded[2 * pair + 1]
            upper = jnp.where(even, one, pltpu.roll(other, SECOND, 1))
            lower = jnp.where(even, pltpu.roll(one, LANES - SECOND, 1), other)
            turned = jnp.concatenate([upper, lower], axis=0).T
            high, low = split_value(turned)
            for side in range(2):
                rows = pl.ds((2 * pair + side) * SECOND, SECOND)
                for half in range(2):
                    start = (2 * half + side) * SECOND
                    piece = high[start:start + SECOND]
                    lhs[rows, pl.ds(half * LANES, LANES)] = piece
                    lhs[rows, pl.ds((2 + half) * LANES, LANES)] = low[start:start + SECOND]
                    lhs[rows, pl.ds((4 + half) * LANES, LANES)] = piece

        cos, sin = mid_ref[0], mid_ref[1]
        results = []
        for group in range(CHUNK // GROUP):
            size = GROUP * SECOND
            section = jnp.dot(lhs[pl.ds(group * size, size), :], one_ref[...],
                              preferred_element_type=jnp.float32)
            for t in range(GROUP):
                real = section[t * SECOND:(t + 1) * SECOND, :FIRST]
                imag = section[t * SECOND:(t + 1) * SECOND, FIRST:]
                for half, value in enumerate((real * cos + imag * sin, imag * cos - real * sin)):
                    high, low = split_value(value)
                    columns = pl.ds(half * FIRST, FIRST)
                    rhs[group, pl.ds(t * SECOND, SECOND), columns] = high
                    rhs[group, pl.ds(size + t * SECOND, SECOND), columns] = low
                    rhs[group, pl.ds(2 * size + t * SECOND, SECOND), columns] = high
            product = jnp.dot(two_ref[...], rhs[group], preferred_element_type=jnp.float32)
            results.append((product[:size, :FIRST] + product[size:, FIRST:],
                            product[:size, FIRST:] - product[size:, :FIRST]))
        for part in range(2):
            for c in range(SECOND):
                block = jnp.concatenate(
                    [results[group][part][c * GROUP:(c + 1) * GROUP] for group in range(CHUNK // GROUP)], axis=0)
                owner, at = divmod(c * FIRST, width)
                staged[chunk, owner, part, :, pl.ds(at, FIRST)] = block.astype(jnp.bfloat16)

        rows = pl.ds(pl.multiple_of(me * frames + chunk * CHUNK, CHUNK), CHUNK)
        for step in order:
            to = partner(me, step, count)
            pltpu.make_async_remote_copy(
                src_ref=staged.at[chunk, to],
                dst_ref=out_ref.at[:, rows, :],
                send_sem=send_sems.at[step - 1],
                recv_sem=recv_sems.at[step - 1],
                device_id={"tm": to},
                device_id_type=MESH,
            ).start()
        pltpu.make_async_copy(staged.at[chunk, me], out_ref.at[:, rows, :], own_sem).start()
        return carry

    total = chunks - 1 + jnp.where(me < count - 1, 1, 0) + jnp.where(me == 0, 1, 0)
    lax.fori_loop(0, total, chunk_step, 0)

    @pl.when(me < count - 1)
    def _():
        past_copy().wait_send()

    @pl.when(me > 0)
    def _():
        head_copy().wait_send()

    def each_range(device, act):
        first, last = device == 0, device == count - 1
        for chosen, skip, size in (
            (first, 0, frames + CHUNK),
            (last, CHUNK, frames - CHUNK),
            (jnp.logical_not(jnp.logical_or(first, last)), CHUNK, frames),
        ):
            @pl.when(chosen)
            def _():
                act(out_ref.at[:, pl.ds(pl.multiple_of(device * frames + skip, CHUNK), size), :])

    each_range(me, lambda rows: pltpu.make_async_copy(rows, rows, own_sem).wait())
    for step in order:
        to = partner(me, step, count)
        source = to if not count & (count - 1) else lax.rem(me + count - step, count)

        def described(rows):
            return pltpu.make_async_remote_copy(
                src_ref=rows, dst_ref=rows, send_sem=send_sems.at[step - 1],
                recv_sem=recv_sems.at[step - 1], device_id={"tm": to}, device_id_type=MESH)

        each_range(me, lambda rows: described(rows).wait_send())
        each_range(source, lambda rows: described(rows).wait_recv())


def local(count, samples, prototype):
    frames = samples.shape[1] // HOP
    rows = samples.shape[1] // LANES
    interleaved = samples.reshape(2, rows, LANES).transpose(1, 0, 2).reshape(2 * rows, LANES)
    one, middle, two = first_table(), middle_table(), second_table()
    in_hbm = pl.BlockSpec(memory_space=pltpu.HBM)
    anywhere = pl.BlockSpec(memory_space=pl.ANY)
    width = CHANNELS // count
    return pl.pallas_call(
        functools.partial(kernel, count, frames),
        out_shape=pltpu.VMEM((2, frames * count, width), jnp.bfloat16),
        in_specs=[in_hbm] * 5,
        out_specs=anywhere,
        scratch_shapes=[
            pltpu.VMEM((RIM_ROWS + 2 * rows + CHUNK * HOP_ROWS, LANES), jnp.float32),
            pltpu.VMEM(prototype.shape, jnp.float32),
            pltpu.VMEM((ROWS * TAPS, LANES), jnp.float32),
            pltpu.VMEM((TAPS, ROWS, LANES), jnp.float32),
            pltpu.VMEM(one.shape, one.dtype),
            pltpu.VMEM(middle.shape, middle.dtype),
            pltpu.VMEM(two.shape, two.dtype),
            pltpu.VMEM((CHUNK, ROWS, LANES), jnp.float32),
            pltpu.VMEM((CHUNK * SECOND, 6 * LANES), jnp.bfloat16),
            pltpu.VMEM((CHUNK // GROUP, 3 * GROUP * SECOND, 2 * FIRST), jnp.bfloat16),
            pltpu.VMEM((frames // CHUNK + 1, count, 2, CHUNK, width), jnp.bfloat16),
            pltpu.SemaphoreType.DMA((5,)),
            pltpu.SemaphoreType.DMA,
            pltpu.SemaphoreType.DMA((2,)),
            pltpu.SemaphoreType.DMA((2,)),
            pltpu.SemaphoreType.DMA((count - 1,)),
            pltpu.SemaphoreType.DMA((count - 1,)),
        ],
        compiler_params=pltpu.CompilerParams(
            collective_id=0, has_side_effects=True, vmem_limit_bytes=60300000
        ),
    )(interleaved, prototype, jnp.asarray(one), jnp.asarray(middle), jnp.asarray(two))


def solution(mesh):
    count = mesh.shape["tm"]
    placed = (P(None, ("beam", "tm")), P())
    return jax.shard_map(
        functools.partial(local, count), mesh=mesh, in_specs=placed,
        out_specs=P(None, "beam", "tm"), check_vma=False,
    )
```
